32 devices in a mesh: rows: 16 (over z, y, x), layer: 2 (over core).
Axes of the slice: x: 2, y: 2, z: 4, core: 2. Of those that a mesh axis runs over, the one named last changes fastest.
Arguments:
- grads: bfloat16 [2, 2048, 8192], P('layer', 'rows'), may hold values from -180 to 180
- momentum: float32 [2, 2048, 8192], P('layer', 'rows'), may hold values from -6 to 6
- weights: float32 [2, 2048, 8192], P('layer', 'rows'), may hold values from -1.5 to 1.5
Outputs:
- new_weights: float32 [2, 2048, 8192], P('layer', 'rows')
- new_momentum: float32 [2, 2048, 8192], P('layer', 'rows')
The draws below stay inside these ranges and needn't reach their ends.
All inputs are finite; a program needn't handle non-finite values.
Results may differ from the reference program's by a relative error of at most 0.0003.
Values sent between devices are 32-bit elements; how exact they have to be, the bound alone decides.
A program may use at most 128 MiB of HBM per device.

```python
import math
import jax
import jax.numpy as jnp
from jax import lax

LATENT = 2048
HEADS = 32
HD = 256
ITERS = 5
LAYERS = 2


def draw_grads(key, part):
    first_key, second_key, third_key = jax.random.split(jax.random.fold_in(key, 17), 3)
    shape = (LAYERS, LATENT, HEADS * HD)
    base = jnp.clip(jax.random.normal(first_key, shape, jnp.float32), -6.0, 6.0)
    row_scale = jnp.exp(jax.random.uniform(second_key, (LAYERS, LATENT, 1), jnp.float32, 0.0, 1.0) * 0.5 * math.log(10.0))
    column_scale = jnp.exp(jax.random.uniform(third_key, (LAYERS, 1, HEADS * HD), jnp.float32, 0.0, 1.0) * 0.5 * math.log(10.0))
    row_place = jnp.arange(LATENT, dtype=jnp.float32)[None, :, None] / LATENT
    layer_place = jnp.arange(LAYERS, dtype=jnp.float32)[:, None, None] / max(LAYERS - 1, 1)
    ramp = jnp.exp(0.5 * math.log(3.0) * (row_place + layer_place))
    return (base * row_scale * column_scale * ramp).astype(jnp.bfloat16)


def steps_of(own_key, dims, cuts, smallest, top_value):
    loudness = 1.0
    for dim, shards_of in cuts:
        draws = jax.random.uniform(jax.random.fold_in(jax.random.fold_in(own_key, 6), dim), (shards_of,), jnp.float32, smallest / len(cuts), top_value / len(cuts))
        loudness = loudness * jnp.repeat(jnp.exp(draws), dims[dim] // shards_of).reshape((-1,) + (1,) * (len(dims) - 1 - dim))
    return loudness


def scatter_about(key, dims, deviation, bound, cuts=(), kind=jnp.bfloat16):
    values = deviation * jax.random.normal(key, dims, jnp.float32)
    if cuts:
        values = values * steps_of(key, dims, cuts, -0.22, 0.18)
    return jnp.clip(values, -bound, bound).astype(kind)


def setup_inputs(seed: int = 0) -> dict:
    key_list = jax.random.split(jax.random.key(seed), 4)
    return {
        "grads": draw_grads(jax.random.fold_in(key_list[3], 71), 0),
        "momentum": scatter_about(key_list[1], (LAYERS, LATENT, HEADS * HD), 0.5, 6.0, ((0, 2), (1, 16)), jnp.float32),
        "weights": scatter_about(key_list[2], (LAYERS, LATENT, HEADS * HD), 0.1, 1.5, ((0, 2), (1, 16)), jnp.float32),
    }


coef_a = 3.4445
coef_b = -4.775
coef_c = 2.0315

def newton_schulz(blocks):
    first = jnp.einsum('kri,krj->kij', blocks, blocks, precision=lax.Precision.HIGHEST)
    norm = jnp.sqrt(jnp.trace(first, axis1=1, axis2=2))[:, None, None] + 1e-07
    current = blocks / norm
    gram = first / (norm * norm)
    for sweep in range(ITERS):
        if sweep > 0:
            gram = jnp.einsum('kri,krj->kij', current, current, precision=lax.Precision.HIGHEST)
        square = jnp.einsum('kij,kjl->kil', gram, gram, precision=lax.Precision.HIGHEST)
        poly = coef_b * gram + coef_c * square
        current = coef_a * current + jnp.einsum('kri,kij->krj', current, poly, precision=lax.Precision.HIGHEST)
    return current

def one_layer(update):
    blocks = update.reshape(LATENT, HEADS, HD).transpose(1, 0, 2)
    result = newton_schulz(blocks)
    return result.transpose(1, 0, 2).reshape(LATENT, HEADS * HD)

def reference(grads, momentum, weights):
    gradient = grads.astype(jnp.float32)
    total = jnp.sum(gradient * gradient)
    limit = 0.5 * math.sqrt(float(LAYERS * LATENT * HEADS * HD))
    factor = jnp.minimum(1.0, limit / (jnp.sqrt(total) + 1e-06))
    clipped = factor * gradient
    new_momentum = 0.95 * momentum + clipped
    update = clipped + 0.95 * new_momentum
    ortho = lax.map(one_layer, update)
    scale = 0.2 * math.sqrt(float(max(LATENT, HD)))
    new_weights = weights - 0.5 * (scale * ortho + 0.1 * weights)
    return (new_weights, new_momentum)
```

```python
import functools
import math

import jax
import jax.numpy as jnp
from jax import lax
from jax.experimental import pallas as pl
from jax.experimental.pallas import tpu as pltpu
from jax.sharding import PartitionSpec as P

HD = 256
ITERS = 5

coef_a = 3.4445
coef_b = -4.775
coef_c = 2.0315
momentum_decay = 0.95
learn_rate = 0.5
weight_decay = 0.1

HIGHEST = lax.Precision.HIGHEST
MESH = pl.DeviceIdType.MESH


def mm(a, b):
    return jnp.dot(a, b, precision=HIGHEST, preferred_element_type=jnp.float32)


def split(x):
    high = x.astype(jnp.bfloat16)
    low = (x - high.astype(jnp.float32)).astype(jnp.bfloat16)
    return high, low


def polynomial(gram):
    row = lax.broadcasted_iota(jnp.int32, (HD, HD), 0)
    col = lax.broadcasted_iota(jnp.int32, (HD, HD), 1)
    eye = jnp.where(row == col, 1.0, 0.0).astype(jnp.float32)
    trace = jnp.sum(jnp.sum(gram * eye, axis=0, keepdims=True), axis=1, keepdims=True)
    norm = jnp.sqrt(trace) + 1e-07
    a = gram / (norm * norm)
    q = None
    for sweep in range(ITERS):
        p = coef_a * eye + (coef_b * a + coef_c * mm(a, a))
        q = p if q is None else mm(q, p)
        if sweep < ITERS - 1:
            a = mm(mm(a, p), p)
    return q / norm


def exchange_kernel(
    devices, layers, limit, g_ref, m_ref, ret_ref, fac_ref,
    squares, mine, outgoing, held, result,
    square_send, square_recv, out_send, out_recv, back_send, back_recv, own_sem,
):
    rows = g_ref.shape[0]
    heads = g_ref.shape[1] // HD
    per_device = heads // devices
    everyone = devices * layers
    me = lax.axis_index("rows")
    layer = lax.axis_index("layer")
    flat = me * layers + layer

    barrier = pltpu.get_barrier_semaphore()

    @pl.loop(1, everyone)
    def _(k):
        peer = (flat + k) % everyone
        pl.semaphore_signal(
            barrier, inc=1, device_id={"rows": peer // layers, "layer": peer % layers}, device_id_type=MESH
        )

    def add_squares(h, acc):
        x = g_ref[:, pl.ds(pl.multiple_of(h * HD, HD), HD)].astype(jnp.float32)
        return acc + x * x

    acc = lax.fori_loop(0, heads, add_squares, jnp.zeros((rows, HD), jnp.float32))
    acc = acc.reshape(rows // 8, 8, HD).sum(axis=0)
    part = acc[:, :128] + acc[:, 128:]
    mine[...] = part
    squares[flat] = part
    pl.semaphore_wait(barrier, everyone - 1)

    def square_copy(k):
        peer = (flat + k) % everyone
        return pltpu.make_async_remote_copy(
            src_ref=mine,
            dst_ref=squares.at[flat],
            send_sem=square_send.at[k],
            recv_sem=square_recv.at[k],
            device_id={"rows": peer // layers, "layer": peer % layers},
            device_id_type=MESH,
        )

    @pl.loop(1, everyone)
    def _(k):
        square_copy(k).start()

    @pl.loop(1, everyone)
    def _(k):
        square_copy(k).wait_recv()

    total = jnp.sum(squares[...], axis=0)
    total = jnp.sum(jnp.sum(total, axis=0, keepdims=True), axis=1, keepdims=True)
    factor = jnp.minimum(1.0, limit / (jnp.sqrt(total) + 1e-06))
    fac_ref[...] = jnp.broadcast_to(factor, fac_ref.shape)

    def update_of(h):
        columns = pl.ds(pl.multiple_of(h * HD, HD), HD)
        clipped = factor * g_ref[:, columns].astype(jnp.float32)
        new_momentum = momentum_decay * m_ref[:, columns] + clipped
        return clipped + momentum_decay * new_momentum

    def block(d):
        return pl.ds(pl.multiple_of(d * rows, rows), rows)

    def out_copy(j, k):
        d = (me + k) % devices
        return pltpu.make_async_remote_copy(
            src_ref=outgoing.at[d * per_device + j],
            dst_ref=held.at[j, block(me)],
            send_sem=out_send.at[j, k],
            recv_sem=out_recv.at[j, k],
            device_id={"rows": d},
            device_id_type=MESH,
        )

    def back_copy(j, k):
        d = (me + k) % devices
        head = me * per_device + j
        return pltpu.make_async_remote_copy(
            src_ref=result.at[j, block(d)],
            dst_ref=ret_ref.at[:, pl.ds(pl.multiple_of(head * HD, HD), HD)],
            send_sem=back_send.at[j, k],
            recv_sem=back_recv.at[j, k],
            device_id={"rows": d},
            device_id_type=MESH,
        )

    def own_copy(j):
        head = me * per_device + j
        return pltpu.make_async_copy(
            result.at[j, block(me)], ret_ref.at[:, pl.ds(pl.multiple_of(head * HD, HD), HD)], own_sem.at[j]
        )

    @pl.loop(0, per_device)
    def _(j):
        @pl.loop(1, devices)
        def _(k):
            h = (me + k) % devices * per_device + j
            outgoing[h] = update_of(h)
            out_copy(j, k).start()

        held[j, block(me), :] = update_of(me * per_device + j)

    @pl.loop(0, per_device)
    def _(j):
        @pl.loop(1, devices)
        def _(k):
            out_copy(j, k).wait_recv()

        step = 2 * rows

        def add_gram(s, gram):
            x = held[j, pl.ds(pl.multiple_of(s * step, step), step), :]
            return gram + lax.dot_general(
                x, x, (((0,), (0,)), ((), ())), precision=HIGHEST, preferred_element_type=jnp.float32
            )

        gram = lax.fori_loop(0, devices // 2, add_gram, jnp.zeros((HD, HD), jnp.float32))
        q_high, q_low = split(polynomial(gram))

        def apply(d):
            high, low = split(held[j, block(d), :])
            dot = functools.partial(jnp.dot, preferred_element_type=jnp.float32)
            result[j, block(d), :] = dot(high, q_high) + (dot(high, q_low) + dot(low, q_high))

        @pl.loop(1, devices)
        def _(k):
            apply((me + k) % devices)
            back_copy(j, k).start()

        apply(me)
        own_copy(j).start()

    @pl.loop(0, per_device)
    def _(j):
        own_copy(j).wait()

        @pl.loop(1, devices)
        def _(k):
            back_copy(j, k).wait_recv()
            back_copy(j, k).wait_send()
            out_copy(j, k).wait_send()

    @pl.loop(1, everyone)
    def _(k):
        square_copy(k).wait_send()


def exchange(gradient, momentum, devices, layers, limit):
    rows, width = gradient.shape
    heads = width // HD
    per_device = heads // devices
    everyone = devices * layers
    latent = rows * devices
    dma = pltpu.SemaphoreType.DMA
    return pl.pallas_call(
        functools.partial(exchange_kernel, devices, layers, limit),
        out_shape=(
            jax.ShapeDtypeStruct((rows, width), jnp.float32),
            jax.ShapeDtypeStruct((8, 128), jnp.float32),
        ),
        in_specs=[pl.BlockSpec(memory_space=pltpu.VMEM)] * 2,
        out_specs=(pl.BlockSpec(memory_space=pl.ANY), pl.BlockSpec(memory_space=pltpu.VMEM)),
        scratch_shapes=[
            pltpu.VMEM((everyone, 8, 128), jnp.float32),
            pltpu.VMEM((8, 128), jnp.float32),
            pltpu.VMEM((heads, rows, HD), jnp.float32),
            pltpu.VMEM((per_device, latent, HD), jnp.float32),
            pltpu.VMEM((per_device, latent, HD), jnp.float32),
            dma((everyone,)),
            dma((everyone,)),
            dma((per_device, devices)),
            dma((per_device, devices)),
            dma((per_device, devices)),
            dma((per_device, devices)),
            dma((per_device,)),
        ],
        compiler_params=pltpu.CompilerParams(
            collective_id=0, has_side_effects=True, vmem_limit_bytes=48 * 1024 * 1024
        ),
    )(gradient, momentum)


def body(grads, momentum, weights):
    devices, layers = lax.axis_size("rows"), lax.axis_size("layer")
    rows, width = grads.shape[1:]
    limit = 0.5 * math.sqrt(float(layers * devices * rows * width))
    returned, fac = exchange(grads[0], momentum[0], devices, layers, limit)
    new_momentum = momentum_decay * momentum[0] + fac[0, 0] * grads[0].astype(jnp.float32)
    scale = 0.2 * math.sqrt(float(max(devices * rows, HD)))
    new_weights = weights[0] - learn_rate * (scale * returned + weight_decay * weights[0])
    return (new_weights[None], new_momentum[None])


def shared_body(grads, momentum, weights):
    devices = lax.axis_size("rows")
    rows, width = grads.shape[1:]
    heads = width // HD
    gradient = grads[0].astype(jnp.float32)
    total = lax.psum(jnp.sum(gradient * gradient), ("rows", "layer"))
    limit = 0.5 * math.sqrt(float(lax.axis_size("layer") * devices * rows * width))
    factor = jnp.minimum(1.0, limit / (jnp.sqrt(total) + 1e-06))
    clipped = factor * gradient
    new_momentum = momentum_decay * momentum[0] + clipped
    update = clipped + momentum_decay * new_momentum
    sharers = devices // heads
    part = rows // sharers
    head_major = update.reshape(rows, heads, HD).transpose(1, 0, 2)
    outgoing = jnp.concatenate([head_major] * sharers, axis=0)
    pieces = lax.all_to_all(outgoing, "rows", split_axis=0, concat_axis=1, tiled=True)
    x = pieces[0]
    gram = lax.dot_general(x, x, (((0,), (0,)), ((), ())), precision=HIGHEST)
    result = mm(x, polynomial(gram))
    side = lax.axis_index("rows") // heads
    shares = result.reshape(devices, sharers, part, HD)
    chosen = lax.dynamic_index_in_dim(shares, side, 1, keepdims=False)
    returned = lax.all_to_all(chosen, "rows", split_axis=0, concat_axis=0, tiled=True)
    returned = returned.reshape(sharers, heads, part, HD).transpose(0, 2, 1, 3).reshape(rows, width)
    scale = 0.2 * math.sqrt(float(max(devices * rows, HD)))
    new_weights = weights[0] - learn_rate * (scale * returned + weight_decay * weights[0])
    return (new_weights[None], new_momentum[None])


def solution(mesh):
    placed = P("layer", "rows", None)

    def step(grads, momentum, weights):
        heads = grads.shape[2] // HD
        chosen = body if heads % mesh.shape["rows"] == 0 else shared_body
        return jax.shard_map(
            chosen, mesh=mesh, in_specs=(placed,) * 3, out_specs=(placed, placed), check_vma=False
        )(grads, momentum, weights)

    return step
```

```python
import functools
import math

import jax
import jax.numpy as jnp
from jax import lax
from jax.experimental import pallas as pl
from jax.experimental.pallas import tpu as pltpu
from jax.sharding import PartitionSpec as P

HD = 256
ITERS = 5

coef_a = 3.4445
coef_b = -4.775
coef_c = 2.0315
momentum_decay = 0.95
learn_rate = 0.5
weight_decay = 0.1

HIGHEST = lax.Precision.HIGHEST
MESH = pl.DeviceIdType.MESH


def mm(a, b):
    return jnp.dot(a, b, precision=HIGHEST, preferred_element_type=jnp.float32)


def split(x):
    high = x.astype(jnp.bfloat16)
    low = (x - high.astype(jnp.float32)).astype(jnp.bfloat16)
    return high, low


def polynomial(gram):
    row = lax.broadcasted_iota(jnp.int32, (HD, HD), 0)
    col = lax.broadcasted_iota(jnp.int32, (HD, HD), 1)
    eye = jnp.where(row == col, 1.0, 0.0).astype(jnp.float32)
    trace = jnp.sum(jnp.sum(gram * eye, axis=0, keepdims=True), axis=1, keepdims=True)
    norm = jnp.sqrt(trace) + 1e-07
    a = gram / (norm * norm)
    q = None
    for sweep in range(ITERS):
        p = coef_a * eye + (coef_b * a + coef_c * mm(a, a))
        q = p if q is None else mm(q, p)
        if sweep < ITERS - 1:
            a = mm(mm(a, p), p)
    return q / norm


def pack(x):
    half = HD // 2
    return jnp.stack([x[:half, :half], x[:half, half:], x[half:, half:]])


def unpack(x):
    top = jnp.concatenate([x[0], x[1]], axis=1)
    return jnp.concatenate([top, jnp.concatenate([x[1].T, x[2]], axis=1)], axis=0)


def exchange_kernel(
    plane, devices, layers, limit, g_ref, m_ref, ret_ref, fac_ref,
    squares, mine, outgoing, held, result, gram_out, grams, own_q, qs,
    square_send, square_recv, out_send, out_recv, back_send, back_recv,
    gram_send, gram_recv, q_send, q_recv, own_sem,
):
    rows = g_ref.shape[0]
    heads = g_ref.shape[1] // HD
    depth = devices // plane
    per_device = heads // devices
    per_plane = heads // plane
    everyone = devices * layers
    me = lax.axis_index("rows")
    layer = lax.axis_index("layer")
    flat = me * layers + layer
    z, p = me // plane, me % plane

    barrier = pltpu.get_barrier_semaphore()

    @pl.loop(1, everyone)
    def _(k):
        peer = (flat + k) % everyone
        pl.semaphore_signal(
            barrier, inc=1, device_id={"rows": peer // layers, "layer": peer % layers}, device_id_type=MESH
        )

    def add_squares(h, acc):
        x = g_ref[:, pl.ds(pl.multiple_of(h * HD, HD), HD)].astype(jnp.float32)
        return acc + x * x

    acc = lax.fori_loop(0, heads, add_squares, jnp.zeros((rows, HD), jnp.float32))
    acc = acc.reshape(rows // 8, 8, HD).sum(axis=0)
    part = acc[:, :128] + acc[:, 128:]
    mine[...] = part
    squares[flat] = part
    pl.semaphore_wait(barrier, everyone - 1)

    def square_copy(k):
        peer = (flat + k) % everyone
        return pltpu.make_async_remote_copy(
            src_ref=mine,
            dst_ref=squares.at[flat],
            send_sem=square_send.at[k],
            recv_sem=square_recv.at[k],
            device_id={"rows": peer // layers, "layer": peer % layers},
            device_id_type=MESH,
        )

    @pl.loop(1, everyone)
    def _(k):
        square_copy(k).start()

    @pl.loop(1, everyone)
    def _(k):
        square_copy(k).wait_recv()

    total = jnp.sum(squares[...], axis=0)
    total = jnp.sum(jnp.sum(total, axis=0, keepdims=True), axis=1, keepdims=True)
    factor = jnp.minimum(1.0, limit / (jnp.sqrt(total) + 1e-06))
    fac_ref[...] = jnp.broadcast_to(factor, fac_ref.shape)

    def columns_of(h):
        return pl.ds(pl.multiple_of(h * HD, HD), HD)

    def update_of(h):
        clipped = factor * g_ref[:, columns_of(h)].astype(jnp.float32)
        new_momentum = momentum_decay * m_ref[:, columns_of(h)] + clipped
        return clipped + momentum_decay * new_momentum

    def block(d):
        return pl.ds(pl.multiple_of(d * rows, rows), rows)

    def chunk(j, kz):
        return j * depth + (z + kz) % depth

    def out_copy(j, kz, kp):
        d = (p + kp) % plane
        c = chunk(j, kz)
        return pltpu.make_async_remote_copy(
            src_ref=outgoing.at[d * per_plane + c],
            dst_ref=held.at[c, block(p)],
            send_sem=out_send.at[j, kz, kp],
            recv_sem=out_recv.at[j, kz, kp],
            device_id={"rows": z * plane + d},
            device_id_type=MESH,
        )

    def back_copy(j, kz, kp):
        d = (p + kp) % plane
        c = chunk(j, kz)
        return pltpu.make_async_remote_copy(
            src_ref=result.at[c, block(d)],
            dst_ref=ret_ref.at[:, columns_of(p * per_plane + c)],
            send_sem=back_send.at[j, kz, kp],
            recv_sem=back_recv.at[j, kz, kp],
            device_id={"rows": z * plane + d},
            device_id_type=MESH,
        )

    def own_copy(j, kz):
        c = chunk(j, kz)
        return pltpu.make_async_copy(
            result.at[c, block(p)], ret_ref.at[:, columns_of(p * per_plane + c)], own_sem.at[j, kz]
        )

    def gram_copy(j, kz):
        return pltpu.make_async_remote_copy(
            src_ref=gram_out.at[chunk(j, kz)],
            dst_ref=grams.at[j, z],
            send_sem=gram_send.at[j, kz],
            recv_sem=gram_recv.at[j, kz],
            device_id={"rows": (z + kz) % depth * plane + p},
            device_id_type=MESH,
        )

    def q_copy(j, kz):
        return pltpu.make_async_remote_copy(
            src_ref=own_q.at[j],
            dst_ref=qs.at[j, z],
            send_sem=q_send.at[j, kz],
            recv_sem=q_recv.at[j, kz],
            device_id={"rows": (z + kz) % depth * plane + p},
            device_id_type=MESH,
        )

    def send_update(j):
        @pl.loop(0, depth)
        def _(i):
            kz = (i + 1) % depth
            c = chunk(j, kz)

            @pl.loop(1, plane)
            def _(kp):
                h = (p + kp) % plane * per_plane + c
                outgoing[h] = update_of(h)
                out_copy(j, kz, kp).start()

            held[c, block(p), :] = update_of(p * per_plane + c)

    def send_gram(j):
        @pl.loop(0, depth)
        def _(i):
            kz = (i + 1) % depth

            @pl.loop(1, plane)
            def _(kp):
                out_copy(j, kz, kp).wait_recv()

            x = held[chunk(j, kz)]
            packed = pack(
                lax.dot_general(
                    x, x, (((0,), (0,)), ((), ())), precision=HIGHEST, preferred_element_type=jnp.float32
                )
            )

            @pl.when(kz != 0)
            def _():
                gram_out[chunk(j, kz)] = packed
                gram_copy(j, kz).start()

            @pl.when(kz == 0)
            def _():
                grams[j, z] = packed

    def send_q(j):
        @pl.loop(1, depth)
        def _(kz):
            gram_copy(j, kz).wait_recv()

        packed = pack(polynomial(unpack(jnp.sum(grams[j], axis=0))))
        own_q[j] = packed
        qs[j, z] = packed

        @pl.loop(1, depth)
        def _(kz):
            q_copy(j, kz).start()

    def send_result(j):
        @pl.loop(0, depth)
        def _(i):
            kz = (depth - i) % depth

            @pl.when(i != 0)
            def _():
                q_copy(j, i).wait_recv()

            c = chunk(j, kz)
            q_high, q_low = split(unpack(qs[j, (z + kz) % depth]))
            high, low = split(held[c])
            dot = functools.partial(jnp.dot, preferred_element_type=jnp.float32)
            result[c] = dot(high, q_high) + (dot(high, q_low) + dot(low, q_high))

            @pl.loop(1, plane)
            def _(kp):
                back_copy(j, kz, kp).start()

            own_copy(j, kz).start()

    for j in range(per_device):
        send_update(j)
    for j in range(per_device):
        send_gram(j)
        if j > 0:
            send_result(j - 1)
        send_q(j)
    send_result(per_device - 1)

    @pl.loop(0, per_device)
    def _(j):
        @pl.loop(0, depth)
        def _(kz):
            own_copy(j, kz).wait()

            @pl.loop(1, plane)
            def _(kp):
                back_copy(j, kz, kp).wait_recv()
                back_copy(j, kz, kp).wait_send()
                out_copy(j, kz, kp).wait_send()

        @pl.loop(1, depth)
        def _(kz):
            gram_copy(j, kz).wait_send()
            q_copy(j, kz).wait_send()

    @pl.loop(1, everyone)
    def _(k):
        square_copy(k).wait_send()


def exchange(gradient, momentum, devices, layers, limit):
    rows, width = gradient.shape
    heads = width // HD
    plane = math.gcd(devices, 1 << (devices.bit_length() // 2))
    depth = devices // plane
    per_device = heads // devices
    per_plane = heads // plane
    everyone = devices * layers
    dma = pltpu.SemaphoreType.DMA
    vmem = lambda *shape: pltpu.VMEM(shape, jnp.float32)
    packed = (3, HD // 2, HD // 2)
    return pl.pallas_call(
        functools.partial(exchange_kernel, plane, devices, layers, limit),
        out_shape=(
            jax.ShapeDtypeStruct((rows, width), jnp.float32),
            jax.ShapeDtypeStruct((8, 128), jnp.float32),
        ),
        in_specs=[pl.BlockSpec(memory_space=pltpu.VMEM)] * 2,
        out_specs=(pl.BlockSpec(memory_space=pl.ANY), pl.BlockSpec(memory_space=pltpu.VMEM)),
        scratch_shapes=[
            vmem(everyone, 8, 128),
            vmem(8, 128),
            vmem(heads, rows, HD),
            vmem(per_plane, plane * rows, HD),
            vmem(per_plane, plane * rows, HD),
            vmem(per_plane, *packed),
            vmem(per_device, depth, *packed),
            vmem(per_device, *packed),
            vmem(per_device, depth, *packed),
            dma((everyone,)),
            dma((everyone,)),
            dma((per_device, depth, plane)),
            dma((per_device, depth, plane)),
            dma((per_device, depth, plane)),
            dma((per_device, depth, plane)),
            dma((per_device, depth)),
            dma((per_device, depth)),
            dma((per_device, depth)),
            dma((per_device, depth)),
            dma((per_device, depth)),
        ],
        compiler_params=pltpu.CompilerParams(
            collective_id=0, has_side_effects=True, vmem_limit_bytes=48 * 1024 * 1024
        ),
    )(gradient, momentum)


def body(grads, momentum, weights):
    devices, layers = lax.axis_size("rows"), lax.axis_size("layer")
    rows, width = grads.shape[1:]
    limit = 0.5 * math.sqrt(float(layers * devices * rows * width))
    returned, fac = exchange(grads[0], momentum[0], devices, layers, limit)
    new_momentum = momentum_decay * momentum[0] + fac[0, 0] * grads[0].astype(jnp.float32)
    scale = 0.2 * math.sqrt(float(max(devices * rows, HD)))
    new_weights = weights[0] - learn_rate * (scale * returned + weight_decay * weights[0])
    return (new_weights[None], new_momentum[None])


def shared_body(grads, momentum, weights):
    devices = lax.axis_size("rows")
    rows, width = grads.shape[1:]
    heads = width // HD
    gradient = grads[0].astype(jnp.float32)
    total = lax.psum(jnp.sum(gradient * gradient), ("rows", "layer"))
    limit = 0.5 * math.sqrt(float(lax.axis_size("layer") * devices * rows * width))
    factor = jnp.minimum(1.0, limit / (jnp.sqrt(total) + 1e-06))
    clipped = factor * gradient
    new_momentum = momentum_decay * momentum[0] + clipped
    update = clipped + momentum_decay * new_momentum
    sharers = devices // heads
    part = rows // sharers
    head_major = update.reshape(rows, heads, HD).transpose(1, 0, 2)
    outgoing = jnp.concatenate([head_major] * sharers, axis=0)
    pieces = lax.all_to_all(outgoing, "rows", split_axis=0, concat_axis=1, tiled=True)
    x = pieces[0]
    gram = lax.dot_general(x, x, (((0,), (0,)), ((), ())), precision=HIGHEST)
    result = mm(x, polynomial(gram))
    side = lax.axis_index("rows") // heads
    shares = result.reshape(devices, sharers, part, HD)
    chosen = lax.dynamic_index_in_dim(shares, side, 1, keepdims=False)
    returned = lax.all_to_all(chosen, "rows", split_axis=0, concat_axis=0, tiled=True)
    returned = returned.reshape(sharers, heads, part, HD).transpose(0, 2, 1, 3).reshape(rows, width)
    scale = 0.2 * math.sqrt(float(max(devices * rows, HD)))
    new_weights = weights[0] - learn_rate * (scale * returned + weight_decay * weights[0])
    return (new_weights[None], new_momentum[None])


def solution(mesh):
    placed = P("layer", "rows", None)

    def step(grads, momentum, weights):
        heads = grads.shape[2] // HD
        chosen = body if heads % mesh.shape["rows"] == 0 else shared_body
        return jax.shard_map(
            chosen, mesh=mesh, in_specs=(placed,) * 3, out_specs=(placed, placed), check_vma=False
        )(grads, momentum, weights)

    return step
```

```python
import functools
import math

import jax
import jax.numpy as jnp
from jax import lax
from jax.experimental import pallas as pl
from jax.experimental.pallas import tpu as pltpu
from jax.sharding import PartitionSpec as P

HD = 256
ITERS = 5

coef_a = 3.4445
coef_b = -4.775
coef_c = 2.0315
momentum_decay = 0.95
learn_rate = 0.5
weight_decay = 0.1

HIGHEST = lax.Precision.HIGHEST
MESH = pl.DeviceIdType.MESH


def mm(a, b):
    return jnp.dot(a, b, precision=HIGHEST, preferred_element_type=jnp.float32)


def split(x):
    high = x.astype(jnp.bfloat16)
    low = (x - high.astype(jnp.float32)).astype(jnp.bfloat16)
    return high, low


def polynomial(gram):
    row = lax.broadcasted_iota(jnp.int32, (HD, HD), 0)
    col = lax.broadcasted_iota(jnp.int32, (HD, HD), 1)
    eye = jnp.where(row == col, 1.0, 0.0).astype(jnp.float32)
    trace = jnp.sum(jnp.sum(gram * eye, axis=0, keepdims=True), axis=1, keepdims=True)
    norm = jnp.sqrt(trace) + 1e-07
    a = gram / (norm * norm)
    q = None
    for sweep in range(ITERS):
        p = coef_a * eye + (coef_b * a + coef_c * mm(a, a))
        q = p if q is None else mm(q, p)
        if sweep < ITERS - 1:
            a = mm(mm(a, p), p)
    return q / norm


def pack(x):
    half = HD // 2
    return jnp.stack([x[:half, :half], x[:half, half:], x[half:, half:]])


def unpack(x):
    top = jnp.concatenate([x[0], x[1]], axis=1)
    return jnp.concatenate([top, jnp.concatenate([x[1].T, x[2]], axis=1)], axis=0)


def exchange_kernel(
    plane, devices, layers, limit, scale, g_ref, m_hbm, w_hbm, new_w_ref, new_m_ref,
    m_ref, w_ref, returned, squares, mine, outgoing, held, result, gram_out, grams, own_q, qs,
    square_send, square_recv, out_send, out_recv, back_send, back_recv,
    gram_send, gram_recv, q_send, q_recv, load_sem,
):
    rows = g_ref.shape[0]
    heads = g_ref.shape[1] // HD
    depth = devices // plane
    per_device = heads // devices
    per_plane = heads // plane
    everyone = devices * layers
    me = lax.axis_index("rows")
    layer = lax.axis_index("layer")
    flat = me * layers + layer
    z, p = me // plane, me % plane

    load_m = pltpu.make_async_copy(m_hbm, m_ref, load_sem.at[0])
    load_w = pltpu.make_async_copy(w_hbm, w_ref, load_sem.at[1])
    load_m.start()
    load_w.start()
    barrier = pltpu.get_barrier_semaphore()

    @pl.loop(1, everyone)
    def _(k):
        peer = (flat + k) % everyone
        pl.semaphore_signal(
            barrier, inc=1, device_id={"rows": peer // layers, "layer": peer % layers}, device_id_type=MESH
        )

    def add_squares(h, acc):
        x = g_ref[:, pl.ds(pl.multiple_of(h * HD, HD), HD)].astype(jnp.float32)
        return acc + x * x

    acc = lax.fori_loop(0, heads, add_squares, jnp.zeros((rows, HD), jnp.float32))
    acc = acc.reshape(rows // 8, 8, HD).sum(axis=0)
    part = acc[:, :128] + acc[:, 128:]
    mine[...] = part
    squares[flat] = part
    pl.semaphore_wait(barrier, everyone - 1)

    def square_copy(k):
        peer = (flat + k) % everyone
        return pltpu.make_async_remote_copy(
            src_ref=mine,
            dst_ref=squares.at[flat],
            send_sem=square_send.at[k],
            recv_sem=square_recv.at[k],
            device_id={"rows": peer // layers, "layer": peer % layers},
            device_id_type=MESH,
        )

    @pl.loop(1, everyone)
    def _(k):
        square_copy(k).start()

    @pl.loop(1, everyone)
    def _(k):
        square_copy(k).wait_recv()

    total = jnp.sum(squares[...], axis=0)
    total = jnp.sum(jnp.sum(total, axis=0, keepdims=True), axis=1, keepdims=True)
    factor = jnp.minimum(1.0, limit / (jnp.sqrt(total) + 1e-06))
    load_m.wait()
    load_w.wait()

    def columns_of(h):
        return pl.ds(pl.multiple_of(h * HD, HD), HD)

    def update_of(h):
        clipped = factor * g_ref[:, columns_of(h)].astype(jnp.float32)
        new_momentum = momentum_decay * m_ref[:, columns_of(h)] + clipped
        new_m_ref[:, columns_of(h)] = new_momentum
        return clipped + momentum_decay * new_momentum

    def block(d):
        return pl.ds(pl.multiple_of(d * rows, rows), rows)

    def chunk(j, kz):
        return j * depth + (z + kz) % depth

    def out_copy(j, kz, kp):
        d = (p + kp) % plane
        c = chunk(j, kz)
        return pltpu.make_async_remote_copy(
            src_ref=outgoing.at[d * per_plane + c],
            dst_ref=held.at[c, block(p)],
            send_sem=out_send.at[j, kz, kp],
            recv_sem=out_recv.at[j, kz, kp],
            device_id={"rows": z * plane + d},
            device_id_type=MESH,
        )

    def back_copy(j, kz, kp):
        d = (p + kp) % plane
        c = chunk(j, kz)
        return pltpu.make_async_remote_copy(
            src_ref=result.at[c, block(d)],
            dst_ref=returned.at[p * per_plane + c],
            send_sem=back_send.at[j, kz, kp],
            recv_sem=back_recv.at[j, kz, kp],
            device_id={"rows": z * plane + d},
            device_id_type=MESH,
        )

    def finish(h, ortho):
        w = w_ref[:, columns_of(h)]
        new_w_ref[:, columns_of(h)] = w - learn_rate * (scale * ortho + weight_decay * w)

    def gram_copy(j, kz):
        return pltpu.make_async_remote_copy(
            src_ref=gram_out.at[chunk(j, kz)],
            dst_ref=grams.at[j, z],
            send_sem=gram_send.at[j, kz],
            recv_sem=gram_recv.at[j, kz],
            device_id={"rows": (z + kz) % depth * plane + p},
            device_id_type=MESH,
        )

    def q_copy(j, kz):
        return pltpu.make_async_remote_copy(
            src_ref=own_q.at[j],
            dst_ref=qs.at[j, z],
            send_sem=q_send.at[j, kz],
            recv_sem=q_recv.at[j, kz],
            device_id={"rows": (z + kz) % depth * plane + p},
            device_id_type=MESH,
        )

    def send_update(j):
        @pl.loop(0, depth)
        def _(i):
            kz = (i + 1) % depth
            c = chunk(j, kz)

            @pl.loop(1, plane)
            def _(kp):
                h = (p + kp) % plane * per_plane + c
                outgoing[h] = update_of(h)
                out_copy(j, kz, kp).start()

            held[c, block(p), :] = update_of(p * per_plane + c)

    def send_gram(j):
        @pl.loop(0, depth)
        def _(i):
            kz = (i + 1) % depth

            @pl.loop(1, plane)
            def _(kp):
                out_copy(j, kz, kp).wait_recv()

            x = held[chunk(j, kz)]
            packed = pack(
                lax.dot_general(
                    x, x, (((0,), (0,)), ((), ())), precision=HIGHEST, preferred_element_type=jnp.float32
                )
            )

            @pl.when(kz != 0)
            def _():
                gram_out[chunk(j, kz)] = packed
                gram_copy(j, kz).start()

            @pl.when(kz == 0)
            def _():
                grams[j, z] = packed

    def send_q(j):
        @pl.loop(1, depth)
        def _(kz):
            gram_copy(j, kz).wait_recv()

        packed = pack(polynomial(unpack(jnp.sum(grams[j], axis=0))))
        own_q[j] = packed
        qs[j, z] = packed

        @pl.loop(1, depth)
        def _(kz):
            q_copy(j, kz).start()

    def send_result(j):
        @pl.loop(0, depth)
        def _(i):
            kz = (depth - i) % depth

            @pl.when(i != 0)
            def _():
                q_copy(j, i).wait_recv()

            c = chunk(j, kz)
            q_high, q_low = split(unpack(qs[j, (z + kz) % depth]))
            high, low = split(held[c])
            dot = functools.partial(jnp.dot, preferred_element_type=jnp.float32)
            result[c] = dot(high, q_high) + (dot(high, q_low) + dot(low, q_high))

            @pl.loop(1, plane)
            def _(kp):
                back_copy(j, kz, kp).start()

            finish(p * per_plane + c, result[c, block(p), :])

    for j in range(per_device):
        send_update(j)
    for j in range(per_device):
        send_gram(j)
        if j > 0:
            send_result(j - 1)
        send_q(j)
    send_result(per_device - 1)

    @pl.loop(0, per_device)
    def _(j):
        @pl.loop(0, depth)
        def _(i):
            kz = (depth - i) % depth

            @pl.loop(1, plane)
            def _(kp):
                back_copy(j, kz, kp).wait_recv()
                h = (p + plane - kp) % plane * per_plane + chunk(j, kz)
                finish(h, returned[h])

    @pl.loop(0, per_device)
    def _(j):
        @pl.loop(0, depth)
        def _(kz):
            @pl.loop(1, plane)
            def _(kp):
                back_copy(j, kz, kp).wait_send()
                out_copy(j, kz, kp).wait_send()

        @pl.loop(1, depth)
        def _(kz):
            gram_copy(j, kz).wait_send()
            q_copy(j, kz).wait_send()

    @pl.loop(1, everyone)
    def _(k):
        square_copy(k).wait_send()


def exchange(gradient, momentum, weights, devices, layers, limit, scale):
    rows, width = gradient.shape
    heads = width // HD
    plane = math.gcd(devices, 1 << (devices.bit_length() // 2))
    depth = devices // plane
    per_device = heads // devices
    per_plane = heads // plane
    everyone = devices * layers
    dma = pltpu.SemaphoreType.DMA
    vmem = lambda *shape: pltpu.VMEM(shape, jnp.float32)
    packed = (3, HD // 2, HD // 2)
    return pl.pallas_call(
        functools.partial(exchange_kernel, plane, devices, layers, limit, scale),
        out_shape=(
            jax.ShapeDtypeStruct((rows, width), jnp.float32),
            jax.ShapeDtypeStruct((rows, width), jnp.float32),
        ),
        in_specs=[pl.BlockSpec(memory_space=pltpu.VMEM)] + [pl.BlockSpec(memory_space=pl.ANY)] * 2,
        out_specs=(pl.BlockSpec(memory_space=pltpu.VMEM), pl.BlockSpec(memory_space=pltpu.VMEM)),
        scratch_shapes=[
            vmem(rows, width),
            vmem(rows, width),
            vmem(heads, rows, HD),
            vmem(everyone, 8, 128),
            vmem(8, 128),
            vmem(heads, rows, HD),
            vmem(per_plane, plane * rows, HD),
            vmem(per_plane, plane * rows, HD),
            vmem(per_plane, *packed),
            vmem(per_device, depth, *packed),
            vmem(per_device, *packed),
            vmem(per_device, depth, *packed),
            dma((everyone,)),
            dma((everyone,)),
            dma((per_device, depth, plane)),
            dma((per_device, depth, plane)),
            dma((per_device, depth, plane)),
            dma((per_device, depth, plane)),
            dma((per_device, depth)),
            dma((per_device, depth)),
            dma((per_device, depth)),
            dma((per_device, depth)),
            dma((2,)),
        ],
        compiler_params=pltpu.CompilerParams(
            collective_id=0, has_side_effects=True, vmem_limit_bytes=40 * 1024 * 1024
        ),
    )(gradient, momentum, weights)


def body(grads, momentum, weights):
    devices, layers = lax.axis_size("rows"), lax.axis_size("layer")
    rows, width = grads.shape[1:]
    limit = 0.5 * math.sqrt(float(layers * devices * rows * width))
    scale = 0.2 * math.sqrt(float(max(devices * rows, HD)))
    new_weights, new_momentum = exchange(grads[0], momentum[0], weights[0], devices, layers, limit, scale)
    return (new_weights[None], new_momentum[None])


def shared_body(grads, momentum, weights):
    devices = lax.axis_size("rows")
    rows, width = grads.shape[1:]
    heads = width // HD
    gradient = grads[0].astype(jnp.float32)
    total = lax.psum(jnp.sum(gradient * gradient), ("rows", "layer"))
    limit = 0.5 * math.sqrt(float(lax.axis_size("layer") * devices * rows * width))
    factor = jnp.minimum(1.0, limit / (jnp.sqrt(total) + 1e-06))
    clipped = factor * gradient
    new_momentum = momentum_decay * momentum[0] + clipped
    update = clipped + momentum_decay * new_momentum
    sharers = devices // heads
    part = rows // sharers
    head_major = update.reshape(rows, heads, HD).transpose(1, 0, 2)
    outgoing = jnp.concatenate([head_major] * sharers, axis=0)
    pieces = lax.all_to_all(outgoing, "rows", split_axis=0, concat_axis=1, tiled=True)
    x = pieces[0]
    gram = lax.dot_general(x, x, (((0,), (0,)), ((), ())), precision=HIGHEST)
    result = mm(x, polynomial(gram))
    side = lax.axis_index("rows") // heads
    shares = result.reshape(devices, sharers, part, HD)
    chosen = lax.dynamic_index_in_dim(shares, side, 1, keepdims=False)
    returned = lax.all_to_all(chosen, "rows", split_axis=0, concat_axis=0, tiled=True)
    returned = returned.reshape(sharers, heads, part, HD).transpose(0, 2, 1, 3).reshape(rows, width)
    scale = 0.2 * math.sqrt(float(max(devices * rows, HD)))
    new_weights = weights[0] - learn_rate * (scale * returned + weight_decay * weights[0])
    return (new_weights[None], new_momentum[None])


def solution(mesh):
    placed = P("layer", "rows", None)

    def step(grads, momentum, weights):
        heads = grads.shape[2] // HD
        chosen = body if heads % mesh.shape["rows"] == 0 else shared_body
        return jax.shard_map(
            chosen, mesh=mesh, in_specs=(placed,) * 3, out_specs=(placed, placed), check_vma=False
        )(grads, momentum, weights)

    return step
```
